32 devices in a mesh: pole: 4 (over x, core), row: 4 (over z), col: 2 (over y).
Axes of the slice: x: 2, y: 2, z: 4, core: 2. Of those that a mesh axis runs over, the one named last changes fastest.
Arguments:
- anc_inverse: bfloat16 [4, 2, 4, 192, 768], P('pole', None, None, 'col', 'row'), may hold values from -6 to 6
- panel: bfloat16 [4, 2, 768, 1024], P('pole', None, ('row', 'col')), may hold values from -0.21875 to 0.21875
- pattern: int32 [8, 2], replicated, may hold values 0 or 1
- diag_inverse: bfloat16 [4, 2, 1024, 512], P('pole', None, 'col', 'row'), may hold values from -6 to 6
- pole_weights: float32 [4, 2], P('pole'), may hold values from -4 to 4
Outputs:
- inv_panel: float32 [4, 2, 768, 1024], P('pole', None, 'row', 'col')
- inv_diag: bfloat16 [4, 2, 1024, 512], P('pole', None, 'col', 'row')
- density: float32 [1024, 512], P('col', 'row')
The draws below stay inside these ranges and needn't reach their ends.
All inputs are finite; a program needn't handle non-finite values.
Results may differ from the reference program's by a relative error of at most 0.013.
Values may be sent and summed in bfloat16 or wider, within the bound.
A program may use at most 128 MiB of HBM per device.

```python
import jax
import jax.numpy as jnp
from jax import lax

W = 512
ANC_DEV = 96
POLES = 4
NK = 2
KW = 1024
NFB = 8
NA = 768
NQ = 4


def plant(values, rng, smallest, high):
    place = [jax.random.randint(jax.random.fold_in(rng, axis), (), 0, length) for axis, length in enumerate(values.shape)]
    main_axis = values.shape.index(max(values.shape))
    next_to = place[:main_axis] + [(place[main_axis] + 1) % values.shape[main_axis]] + place[main_axis + 1:]
    return values.at[tuple(place)].set(smallest).at[tuple(next_to)].set(high)


def block_scale(key, dims, pieces, smallest, top_value):
    factor_of = 1.0
    for axis_at, blocks in pieces:
        steps = jax.random.uniform(jax.random.fold_in(jax.random.fold_in(key, 6), axis_at), (blocks,), jnp.float32, smallest / len(pieces), top_value / len(pieces))
        factor_of = factor_of * jnp.repeat(jnp.exp(steps), dims[axis_at] // blocks).reshape((-1,) + (1,) * (len(dims) - 1 - axis_at))
    return factor_of


def bell_draw(own_key, dims, spread, most, split=(), held_as=jnp.bfloat16):
    loudness = block_scale(own_key, dims, split, -0.22, 0.18) if split else 1.0
    values = jax.random.normal(own_key, dims, jnp.float32) * spread * loudness
    return jnp.minimum(jnp.maximum(values, -most), most).astype(held_as)


def setup_inputs(seed: int = 0) -> dict:
    splits = jax.random.split(jax.random.key(seed), 6)
    return {
        "anc_inverse": bell_draw(splits[0], (POLES, 2, NQ, NA // NQ, NA), 1.0, 6.0, ((0, 4), (3, 2), (4, 4))),
        "panel": bell_draw(splits[1], (POLES, 2, NA, KW), NA ** -0.5, 0.21875, ((0, 4), (2, 8))),
        "pattern": plant((jax.random.randint(splits[2], (NFB, NK), 0, 3) < 2).astype(jnp.int32), jax.random.fold_in(splits[2], 1), 0, 1),
        "diag_inverse": bell_draw(splits[3], (POLES, 2, KW, W), 1.0, 6.0, ((0, 4), (2, 2), (3, 4))),
        "pole_weights": bell_draw(splits[4], (POLES, 2), 1.0, 4.0, ((0, 4),), jnp.float32),
    }


def complex_product(left_re, left_im, right_re, right_im):
    exact = lax.Precision.HIGHEST
    left_re = left_re.astype(jnp.float32)
    left_im = left_im.astype(jnp.float32)
    right_re = right_re.astype(jnp.float32)
    right_im = right_im.astype(jnp.float32)
    real_part = jnp.dot(left_re.T, right_re, precision=exact) - jnp.dot(left_im.T, right_im, precision=exact)
    imag_part = jnp.dot(left_im.T, right_re, precision=exact) + jnp.dot(left_re.T, right_im, precision=exact)
    return real_part, imag_part


def reference(anc_inverse, panel, pattern, diag_inverse, pole_weights):
    exact = lax.Precision.HIGHEST
    keep_mask = jnp.repeat(jnp.repeat(pattern.astype(jnp.bfloat16), W, axis=1), ANC_DEV, axis=0)

    def contract(first, second):
        return jnp.einsum('jka,jkb->kab', first, second, precision=exact)

    def one_pole(inputs):
        ancestor, factor, diagonal = inputs
        transposed = ancestor.reshape(2, NA, NA)
        masked = factor * keep_mask[None]
        prod_re, prod_im = complex_product(transposed[0], transposed[1], masked[0], masked[1])
        result_panel = jnp.stack([-prod_re, -prod_im])
        rounded = lax.optimization_barrier(result_panel.astype(jnp.bfloat16)).astype(jnp.float32)
        factor_full = masked.astype(jnp.float32).reshape(2, NA, NK, W)
        panel_full = rounded.reshape(2, NA, NK, W)
        diag_re = contract(factor_full[0], panel_full[0]) - contract(factor_full[1], panel_full[1])
        diag_im = contract(factor_full[0], panel_full[1]) + contract(factor_full[1], panel_full[0])
        result_diag = diagonal.astype(jnp.float32) - jnp.stack([diag_re, diag_im]).reshape(2, KW, W)
        return result_panel, result_diag

    inv_panel, diag_full = lax.map(one_pole, (anc_inverse, panel, diag_inverse))
    density = jnp.einsum('p,pab->ab', pole_weights[:, 0], diag_full[:, 1], precision=exact)
    density = density + jnp.einsum('p,pab->ab', pole_weights[:, 1], diag_full[:, 0], precision=exact)
    return inv_panel, diag_full.astype(jnp.bfloat16), density
```

```python
import functools

import jax
import jax.numpy as jnp
from jax import lax
from jax.experimental import pallas as pl
from jax.experimental.pallas import tpu as pltpu
from jax.sharding import PartitionSpec as P

MESH = pl.DeviceIdType.MESH
F32 = jnp.float32
BF16 = jnp.bfloat16


def kernel(
    n_pole, n_row, n_col,
    anc, panel, pattern, diag, weights,
    out_panel, out_diag, out_density,
    buf, gbuf, lhs, psend, pbuf, rhs, dterm, dsend, drecv, xbuf, fsend, frecv,
    s_y, s_up, s_dn, r_ag, s_g, r_g, s_p, r_p, s_d, r_d, s_x, r_x, s_f, r_f,
):
    p, r, c = lax.axis_index("pole"), lax.axis_index("row"), lax.axis_index("col")
    core = lax.rem(p, 2)
    x_me = p // 2
    partner = p + 1 - 2 * core
    n_x = n_pole // 2
    has_up, has_dn = r + 1 < n_row, r > 0
    rows = panel.shape[2]
    width = panel.shape[3] // n_col
    chunk = width // n_row
    i_rows = anc.shape[4]
    n_fine = n_row * n_col
    deep = n_fine * 2 * rows
    order = [0] + list(range(n_row - 1, n_row // 2, -1)) + list(range(1, n_row // 2 + 1))

    def remote(src, dst, send, recv, **where):
        return pltpu.make_async_remote_copy(
            src_ref=src, dst_ref=dst, send_sem=send, recv_sem=recv, device_id=where, device_id_type=MESH
        )

    barrier = pltpu.get_barrier_semaphore()

    def greet(**where):
        pl.semaphore_signal(barrier, inc=1, device_id=where, device_id_type=MESH)

    @pl.when(has_up)
    def _():
        greet(row=r + 1)

    @pl.when(has_dn)
    def _():
        greet(row=r - 1)

    for k in range(1, n_col):
        greet(col=lax.rem(c + k, n_col))
    greet(pole=partner)
    for k in range(1, n_x):
        greet(pole=lax.rem(p + 2 * k, n_pole))
    near = has_up.astype(jnp.int32) + has_dn.astype(jnp.int32)
    pl.semaphore_wait(barrier, near + (n_col - 1) + 1 + (n_x - 1))

    pending = []

    def start(copy, cond=None):
        if cond is None:
            copy.start()
        else:
            pl.when(cond)(copy.start)
        pending.append((copy, cond))

    def cols(col, t):
        return pl.ds(pl.multiple_of(col * width + t * chunk, chunk), chunk)

    def send_y(t):
        for k in range(1, n_col):
            other = lax.rem(c + k, n_col)
            f = r * n_col + c
            start(remote(panel.at[0, :, :, cols(other, t)], buf.at[t, f], s_y.at[t, k - 1], r_ag.at[t, f], col=other))

    def got(t, f):
        piece = buf.at[t, f]
        remote(piece, piece, s_y.at[0, 0], r_ag.at[t, f], col=c).wait_recv()

    def up(t, f, src, cond):
        start(remote(src, buf.at[t, f], s_up.at[t, f], r_ag.at[t, f], row=r + 1), cond)

    def down(t, f, src, cond):
        start(remote(src, buf.at[t, f], s_dn.at[t, f], r_ag.at[t, f], row=r - 1), cond)

    mine = r * n_col + c

    def send_own(t):
        up(t, mine, panel.at[0, :, :, cols(c, t)], has_up)
        down(t, mine, panel.at[0, :, :, cols(c, t)], has_dn)

    def mask(f):
        return pattern[f, c].astype(F32)

    def prepare():
        for k in range(1, n_col):
            f = lax.rem(c + k, n_col)
            remote(anc.at[0], gbuf.at[f], s_g.at[0], r_g.at[f], col=c).wait_recv()
        for q in range(n_row):
            for u in range(0, n_col, 2):
                top, low = [], []
                for v in (u, u + 1):
                    scale = -mask(q * n_col + v)
                    re = gbuf[v, 0, q].astype(F32) * scale
                    im = gbuf[v, 1, q].astype(F32) * scale
                    top += [re, -im]
                    low += [im, re]
                at = (q * n_col + u) * 2 * rows
                lhs[0:i_rows, at:at + 4 * rows] = jnp.concatenate(top, axis=0).T.astype(BF16)
                lhs[i_rows:, at:at + 4 * rows] = jnp.concatenate(low, axis=0).T.astype(BF16)

    def compute(t):
        right = buf[t].reshape(deep, chunk)
        for part in range(2):
            got_part = jnp.dot(lhs[part * i_rows:(part + 1) * i_rows], right, preferred_element_type=F32)
            out_panel[0, part, :, t * chunk:(t + 1) * chunk] = got_part
            rounded = got_part.astype(BF16).astype(F32)
            for v in range(n_col):
                psend[t, v, part] = (rounded[v * rows:(v + 1) * rows] * mask(r * n_col + v)).astype(BF16)

        @pl.when(r == t)
        def _():
            pbuf[t] = psend[t]

        start(remote(psend.at[t], pbuf.at[r], s_p.at[t], r_p.at[r], row=t), r != t)

    send_y(order[0])
    send_own(order[0])
    if n_row > 1:
        send_y(order[1])
    for k in range(1, n_col):
        start(remote(anc.at[0], gbuf.at[c], s_g.at[k - 1], r_g.at[c], col=lax.rem(c + k, n_col)))
    for t in order[2:]:
        send_y(t)
    for t in range(n_row):
        buf[t, mine] = panel[0, :, :, cols(c, t)]
    gbuf[c] = anc[0]

    for s in range(2 * n_row - 1):
        if s < n_row:
            t = order[s]
            if s > 0:
                send_own(t)
            for k in range(1, n_col):
                f = r * n_col + lax.rem(c + k, n_col)
                got(t, f)
                up(t, f, buf.at[t, f], has_up)
                down(t, f, buf.at[t, f], has_dn)
        for d in range(1, n_row):
            if not 0 <= s - d < n_row:
                continue
            t = order[s - d]
            for k in range(n_col):
                v = lax.rem(c + k, n_col)
                below, above = r >= d, r + d < n_row
                f_below, f_above = (r - d) * n_col + v, (r + d) * n_col + v
                pl.when(below)(functools.partial(got, t, f_below))
                up(t, f_below, buf.at[t, f_below], below & has_up)
                pl.when(above)(functools.partial(got, t, f_above))
                down(t, f_above, buf.at[t, f_above], above & has_dn)
        if s == n_row - 2:
            prepare()
        if s >= n_row - 1:
            compute(order[s - n_row + 1])

    for k in range(1, n_row):
        other = lax.rem(r + k, n_row)
        remote(psend.at[0], pbuf.at[other], s_p.at[0], r_p.at[other], row=r).wait_recv()
    for q in range(n_row):
        for v in range(n_col):
            f = q * n_col + v
            re, im = pbuf[q, v, 0], pbuf[q, v, 1]
            rhs[f, 0, :, 0:chunk] = re
            rhs[f, 0, :, chunk:] = im
            rhs[f, 1, :, 0:chunk] = -im
            rhs[f, 1, :, chunk:] = re
    right = rhs[...].reshape(deep, 2 * chunk)
    w_re, w_im = weights[0, 0], weights[0, 1]
    for t in range(n_row):
        part = lax.dot_general(
            buf[t].reshape(deep, chunk), right, (((0,), (0,)), ((), ())), preferred_element_type=F32
        )
        at = slice(t * chunk, (t + 1) * chunk)
        d_re = diag[0, 0, at].astype(F32) - part[:, 0:chunk]
        d_im = diag[0, 1, at].astype(F32) - part[:, chunk:]
        out_diag[0, 0, at] = d_re.astype(BF16)
        out_diag[0, 1, at] = d_im.astype(BF16)
        term = w_re * d_im + w_im * d_re
        dterm[at] = term
        dsend[at] = term.astype(BF16)

    half = width // 2
    keep = pl.ds(pl.multiple_of(core * half, half), half)
    give = pl.ds(pl.multiple_of((1 - core) * half, half), half)
    swap = remote(dsend.at[give], drecv, s_d, r_d, pole=partner)
    start(swap)
    swap.wait_recv()
    xbuf[x_me] = (dterm[keep] + drecv[...].astype(F32)).astype(BF16)
    for k in range(1, n_x):
        start(remote(xbuf.at[x_me], xbuf.at[x_me], s_x.at[k - 1], r_x.at[x_me], pole=lax.rem(p + 2 * k, n_pole)))
    for k in range(1, n_x):
        other = lax.rem(x_me + k, n_x)
        remote(xbuf.at[other], xbuf.at[other], s_x.at[0], r_x.at[other], pole=p).wait_recv()
    total = xbuf[0].astype(F32)
    for k in range(1, n_x):
        total += xbuf[k].astype(F32)
    fsend[...] = total
    back = remote(fsend, frecv, s_f, r_f, pole=partner)
    start(back)
    out_density[keep] = total
    for copy, cond in pending:
        if cond is None:
            copy.wait_send()
        else:
            pl.when(cond)(copy.wait_send)
    back.wait_recv()
    out_density[give] = frecv[...]


def body(anc_inverse, panel, pattern, diag_inverse, pole_weights):
    n_pole, n_row, n_col = lax.axis_size("pole"), lax.axis_size("row"), lax.axis_size("col")
    rows = panel.shape[2]
    width = panel.shape[3] // n_col
    chunk = width // n_row
    i_rows = anc_inverse.shape[4]
    n_fine = n_row * n_col
    deep = n_fine * 2 * rows
    n_x = n_pole // 2
    half = width // 2
    dma = pltpu.SemaphoreType.DMA
    vmem = pl.BlockSpec(memory_space=pltpu.VMEM)
    smem = pl.BlockSpec(memory_space=pltpu.SMEM)
    return pl.pallas_call(
        functools.partial(kernel, n_pole, n_row, n_col),
        out_shape=(
            jax.ShapeDtypeStruct((1, 2, i_rows, width), F32),
            jax.ShapeDtypeStruct(diag_inverse.shape, BF16),
            jax.ShapeDtypeStruct((width, chunk), F32),
        ),
        in_specs=[vmem, vmem, smem, vmem, smem],
        out_specs=(vmem, vmem, vmem),
        scratch_shapes=[
            pltpu.VMEM((n_row, n_fine, 2, rows, chunk), BF16),
            pltpu.VMEM((n_col, 2, n_row, rows, i_rows), BF16),
            pltpu.VMEM((2 * i_rows, deep), BF16),
            pltpu.VMEM((n_row, n_col, 2, i_rows // n_col, chunk), BF16),
            pltpu.VMEM((n_row, n_col, 2, i_rows // n_col, chunk), BF16),
            pltpu.VMEM((n_fine, 2, rows, 2 * chunk), BF16),
            pltpu.VMEM((width, chunk), F32),
            pltpu.VMEM((width, chunk), BF16),
            pltpu.VMEM((half, chunk), BF16),
            pltpu.VMEM((n_x, half, chunk), BF16),
            pltpu.VMEM((half, chunk), F32),
            pltpu.VMEM((half, chunk), F32),
            dma((n_row, n_col - 1)),
            dma((n_row, n_fine)),
            dma((n_row, n_fine)),
            dma((n_row, n_fine)),
            dma((n_col - 1,)),
            dma((n_col,)),
            dma((n_row,)),
            dma((n_row,)),
            dma,
            dma,
            dma((n_x,)),
            dma((n_x,)),
            dma,
            dma,
        ],
        compiler_params=pltpu.CompilerParams(
            collective_id=0, has_side_effects=True, vmem_limit_bytes=67043328
        ),
    )(anc_inverse, panel, pattern, diag_inverse, pole_weights)


def solution(mesh):
    placed = (
        P("pole", None, None, "col", "row"),
        P("pole", None, ("row", "col"), None),
        P(),
        P("pole", None, "col", "row"),
        P("pole", None),
    )
    return jax.shard_map(
        body,
        mesh=mesh,
        in_specs=placed,
        out_specs=(P("pole", None, "row", "col"), P("pole", None, "col", "row"), P("col", "row")),
        check_vma=False,
    )
```
